256 devices in a mesh: ent: 128 (over x, y, z_lo, core), grp: 2 (over z_hi).
Axes of the slice: x: 4, y: 4, z: 8 (z_hi: 2, z_lo: 4; z = z_hi * 4 + z_lo), core: 2. Of those that a mesh axis runs over, the one named last changes fastest.
Arguments:
- entity_table: bfloat16 [65536, 1024], P('ent'), may hold values from -2.5 to 2.5
- rel_phases: float32 [822, 512], replicated, may hold values from -3.1416 to 3.1416
- head_ids: int32 [65536], P(('ent', 'grp')), may hold values from 0 to 511
- rel_ids: int32 [65536], P(('ent', 'grp')), may hold values from 0 to 821
- target_pos: int32 [65536], P(('ent', 'grp')), may hold values from 0 to 511
- block_owner: int32 [4], replicated, may hold values from 0 to 127
- block_local: int32 [4], replicated, may hold values from 0 to 3
Outputs:
- losses: float32 [65536], P(('ent', 'grp'))
- head_grad: bfloat16 [65536, 1024], P(('ent', 'grp'))
- table_grad: bfloat16 [65536, 1024], P('ent')
- rel_grad: float32 [822, 512], replicated
The draws below stay inside these ranges and needn't reach their ends.
Inputs may be any that keep to these rules, and one draw needn't show every extreme that they name: query q on device d (ent then grp) has head row (d // 2) * 512 + head_ids[q]. `target_pos`: position among the 512 candidates, block after block. Block b covers table rows from (block_owner[b] * 4 + block_local[b]) * 128 on; blocks may repeat.
All inputs are finite; a program needn't handle non-finite values.
Results may differ from the reference program's by a relative error of at most 0.0057.
Values may be sent and summed in bfloat16 or wider, within the bound.
A program may use at most 64 MiB of HBM per device.

```python
import math
import jax
import jax.numpy as jnp
import numpy as np
from jax import lax

K = 512
R = 822
BLK = 128
NBLK = 4
ENT_DEV = 512
Q_DEV = 256
SHARDS = 128
NENT = 65536
QUERIES = 65536
CAND = 512
N_ENT = 128
N_GRP = 2


def draw_entity_table(key, part):
    key_noise = jax.random.fold_in(key, 2)
    values = jnp.clip(0.25 * jax.random.normal(key_noise, (NENT, 2 * K), jnp.float32), -1.5, 1.5)
    return values.astype(jnp.bfloat16)


def draw_rel_phases(key, part):
    return jax.random.uniform(key, (R, K), jnp.float32, -3.1415, 3.1415)


def plant(values, rng, least, high):
    longest = values.shape.index(max(values.shape))
    spots = []
    for shift in (0, 1):
        where = [jax.random.randint(jax.random.fold_in(rng, axis), (), 0, length) for axis, length in enumerate(values.shape)]
        where[longest] = (where[longest] + shift) % values.shape[longest]
        spots.append(tuple(where))
    return values.at[spots[0]].set(least).at[spots[1]].set(high)


def cumulative_ranks(amount, slope):
    portions = [(1 << 20) // math.isqrt(grade ** slope) + 1 for grade in range(1, amount + 1)]
    width = 1 + sum(portions) // (1 << 30)
    return np.cumsum(np.array([max(1, weight // width) for weight in portions]))


def ranked(key, extent, number_of, lean):
    listing = cumulative_ranks(number_of, lean)
    ticket = jax.random.randint(jax.random.fold_in(key, 1), extent, 0, int(listing[number_of - 1]))
    rank = jnp.searchsorted(jnp.asarray(listing, jnp.int32), ticket, side="right")
    return jax.random.permutation(jax.random.fold_in(key, 2), number_of)[rank].astype(jnp.int32)


def setup_inputs(seed: int = 0) -> dict:
    arg_keys = jax.random.split(jax.random.key(seed), 8)
    return {
        "entity_table": draw_entity_table(jax.random.fold_in(arg_keys[7], 71), 0),
        "rel_phases": draw_rel_phases(jax.random.fold_in(arg_keys[7], 71), 0),
        "head_ids": plant(jax.random.randint(arg_keys[2], (QUERIES,), 0, ENT_DEV), jax.random.fold_in(arg_keys[2], 1), 0, ENT_DEV - 1).astype(jnp.int32),
        "rel_ids": plant(ranked(arg_keys[3], (QUERIES,), R, 2), jax.random.fold_in(arg_keys[3], 3), 0, R - 1).astype(jnp.int32),
        "target_pos": plant(jax.random.randint(arg_keys[4], (QUERIES,), 0, CAND), jax.random.fold_in(arg_keys[4], 1), 0, CAND - 1).astype(jnp.int32),
        "block_owner": plant(jax.random.randint(arg_keys[5], (NBLK,), 0, SHARDS), jax.random.fold_in(arg_keys[5], 1), 0, SHARDS - 1).astype(jnp.int32),
        "block_local": plant(jax.random.randint(arg_keys[6], (NBLK,), 0, ENT_DEV // BLK), jax.random.fold_in(arg_keys[6], 1), 0, (ENT_DEV // BLK) - 1).astype(jnp.int32),
    }


SOFTMAX_TEMPER = 2.0


def device_terms(heads, angles, targets, candidate_block, candidate_norm):
    half_dim = angles.shape[1]
    real_head = heads[:, :half_dim]
    imag_head = heads[:, half_dim:]
    cosine = jnp.cos(angles)
    sine = jnp.sin(angles)
    real_query = real_head * cosine - imag_head * sine
    imag_query = real_head * sine + imag_head * cosine
    query_reduced_precision = jnp.concatenate([real_query, imag_query], axis=1).astype(jnp.bfloat16)
    query_reduced_precision = lax.optimization_barrier(query_reduced_precision).astype(jnp.float32)
    logit_scores = (2.0 * jnp.dot(query_reduced_precision, candidate_block.T, precision=lax.Precision.HIGHEST) - candidate_norm[None, :]) / SOFTMAX_TEMPER
    top = jnp.max(logit_scores, axis=1, keepdims=True)
    log_total = top[:, 0] + jnp.log(jnp.sum(jnp.exp(logit_scores - top), axis=1))
    picked = jnp.take_along_axis(logit_scores, targets[:, None], axis=1)[:, 0]
    losses = log_total - picked
    columns = jnp.arange(logit_scores.shape[1], dtype=jnp.int32)
    onehot = (columns[None, :] == targets[:, None]).astype(jnp.float32)
    softmax_weights = jnp.exp(logit_scores - log_total[:, None]) - onehot
    weights_reduced_precision = lax.optimization_barrier(softmax_weights.astype(jnp.bfloat16)).astype(jnp.float32)
    query_gradient = (2.0 / SOFTMAX_TEMPER) * jnp.dot(weights_reduced_precision, candidate_block, precision=lax.Precision.HIGHEST)
    candidate_gradient = (2.0 / SOFTMAX_TEMPER) * (jnp.dot(weights_reduced_precision.T, query_reduced_precision, precision=lax.Precision.HIGHEST) - jnp.sum(softmax_weights, axis=0)[:, None] * candidate_block)
    real_grad = query_gradient[:, :half_dim]
    imag_grad = query_gradient[:, half_dim:]
    head_grad = jnp.concatenate([real_grad * cosine + imag_grad * sine, imag_grad * cosine - real_grad * sine], axis=1).astype(jnp.bfloat16)
    angle_grad = imag_grad * real_query - real_grad * imag_query
    return losses, head_grad, angle_grad, candidate_gradient


def reference(entity_table, rel_phases, head_ids, rel_ids, target_pos, block_owner, block_local):
    half_dim = rel_phases.shape[1]
    rel_count = rel_phases.shape[0]
    devices = N_ENT * N_GRP
    starts = (block_owner * (ENT_DEV // BLK) + block_local) * BLK
    rows = (starts[:, None] + jnp.arange(BLK, dtype=jnp.int32)[None, :]).reshape(-1).astype(jnp.int32)
    candidate_block = entity_table[rows].astype(jnp.float32)
    candidate_norm = jnp.sum(candidate_block * candidate_block, axis=1)

    def step(carry, inputs):
        cand_total, rel_total = carry
        head_local, rel_local, target_local, device = inputs
        head_rows = ((device // N_GRP) * ENT_DEV + head_local).astype(jnp.int32)
        heads = entity_table[head_rows].astype(jnp.float32)
        angles = rel_phases[rel_local]
        losses, head_grad, angle_grad, candidate_gradient = device_terms(heads, angles, target_local, candidate_block, candidate_norm)
        rel_part = jax.ops.segment_sum(angle_grad, rel_local, num_segments=rel_count)
        return (cand_total + candidate_gradient, rel_total + rel_part), (losses, head_grad)

    start_carry = (jnp.zeros((NBLK * BLK, 2 * half_dim), jnp.float32), jnp.zeros((rel_count, half_dim), jnp.float32))
    inputs = (head_ids.reshape(devices, Q_DEV), rel_ids.reshape(devices, Q_DEV), target_pos.reshape(devices, Q_DEV), jnp.arange(devices, dtype=jnp.int32))
    (cand_total, rel_grad), (losses, head_grad) = lax.scan(step, start_carry, inputs)
    table_grad = jax.ops.segment_sum(cand_total, rows, num_segments=NENT).astype(jnp.bfloat16)
    return losses.reshape(-1), head_grad.reshape(-1, 2 * half_dim), table_grad, rel_grad
```

```python
import functools

import jax
import jax.numpy as jnp
from jax import lax
from jax.experimental import pallas as pl
from jax.experimental.pallas import tpu as pltpu
from jax.sharding import PartitionSpec as P

BLK = 128
SOFTMAX_TEMPER = 2.0
MESH = pl.DeviceIdType.MESH
F32 = jnp.float32
BF16 = jnp.bfloat16
CORE, ZLO, YDIM, XDIM = (1, 2), (2, 4), (8, 4), (32, 4)
ORDERS = ((XDIM, YDIM), (YDIM, XDIM))
TILE = 128


class Exchange:
    def __init__(self, refs, base, length, order, sems, place, along_z):
        self.acc, self.stage, self.out, self.swap, self.r0, self.r1, self.rz = refs
        self.base, self.length, self.part = base, length, length // 4
        self.first, self.second = ORDERS[order]
        self.sems = sems
        self.ent, self.grp = place
        self.along_z = along_z
        self.core = lax.rem(self.ent, 2)
        self.sibling = self.ent + 1 - 2 * self.core
        self.mine0 = self.coordinate(*self.first)
        self.mine1 = self.coordinate(*self.second)
        self.all_rows = pl.ds(base, length)
        self.slot_rows = pl.ds(base // 4, self.part)
        self.started = []
        self.live = []
        self.step = 0

    def go(self, src, dst, ent, grp):
        send, recv = self.sems
        number = len(send[1])
        send[1].append(number)
        copy = pltpu.make_async_remote_copy(
            src_ref=src,
            dst_ref=dst,
            send_sem=send[0].at[number],
            recv_sem=recv.at[number],
            device_id=(ent, grp),
            device_id_type=MESH,
        )
        copy.start()
        self.started.append(copy)
        return copy

    def land(self):
        for copy in self.live:
            copy.wait_recv()
        self.live = []

    def coordinate(self, stride, size):
        return lax.rem(self.ent // stride, size)

    def peers(self, dim):
        stride, size = dim
        mine = self.coordinate(stride, size)
        for k in range(1, size):
            theirs = lax.rem(mine + k, size)
            yield theirs, self.ent + (theirs - mine) * stride

    def col(self, number):
        return pl.ds(pl.multiple_of(number * TILE, TILE), TILE)

    def sub(self, number):
        return pl.ds(pl.multiple_of(self.base + number * self.part, 16), self.part)

    def put(self, rows, cols, value):
        self.acc[rows, cols] = value.astype(self.acc.dtype)
        if self.stage is not self.acc:
            self.stage[rows, cols] = value.astype(BF16)

    def swap_start(self):
        src, dst = self.swap
        self.live.append(
            self.go(src.at[self.all_rows, :], dst.at[self.all_rows, :], self.sibling, self.grp)
        )

    def swap_finish(self):
        self.land()
        rows, cols = self.all_rows, slice(None)
        arrived = self.swap[1][rows, :].astype(F32)
        self.put(rows, cols, self.acc[rows, :].astype(F32) + arrived)
        for k, (theirs, peer) in enumerate(self.peers(self.first)):
            src = self.stage.at[rows, self.col(theirs)]
            self.live.append(self.go(src, self.r0.at[k, rows, :], peer, self.grp))

    def scatter_second(self):
        self.land()
        rows, cols = self.all_rows, self.col(self.mine0)
        total = self.acc[rows, cols].astype(F32)
        for k in range(3):
            total = total + self.r0[k, rows, :].astype(F32)
        self.put(rows, cols, total)
        for k, (theirs, peer) in enumerate(self.peers(self.second)):
            src = self.stage.at[self.sub(theirs), cols]
            self.live.append(self.go(src, self.r1.at[k, self.slot_rows, :], peer, self.grp))

    def z_send(self, level, total):
        slots = self.rz[level]
        mine, partners = self.along_z[level]
        slots[mine, self.slot_rows, :] = total.astype(BF16)
        place = slots.at[mine, self.slot_rows, :]
        for ent, grp in partners:
            self.live.append(self.go(place, place, ent, grp))

    def z_sum(self, level):
        self.land()
        slots = self.rz[level]
        total = slots[0, self.slot_rows, :].astype(F32)
        for k in range(1, slots.shape[0]):
            total = total + slots[k, self.slot_rows, :].astype(F32)
        return total

    def z_start(self):
        self.land()
        total = self.acc[self.sub(self.mine1), self.col(self.mine0)].astype(F32)
        for k in range(3):
            total = total + self.r1[k, self.slot_rows, :].astype(F32)
        self.z_send(0, total)

    def z_next(self, level):
        self.z_send(level, self.z_sum(level - 1))

    def piece(self, first, second):
        return self.out.at[self.core, self.sub(second), self.col(first)]

    def spread(self, piece):
        return [self.go(piece, piece, peer, self.grp) for _, peer in self.peers(self.first)]

    def gather_start(self):
        total = self.z_sum(len(self.along_z) - 1)
        self.out[self.core, self.sub(self.mine1), self.col(self.mine0)] = total.astype(BF16)
        piece = self.piece(self.mine0, self.mine1)
        self.near = [self.go(piece, piece, peer, self.grp) for _, peer in self.peers(self.second)]
        self.far = [self.spread(piece)]

    def gather_first(self):
        for k, copy in enumerate(self.near):
            copy.wait_recv()
            theirs = lax.rem(self.mine1 + 3 - k, 4)
            self.far.append(self.spread(self.piece(self.mine0, theirs)))
        self.share(self.mine0)

    def share(self, number):
        block = self.out.at[self.core, self.all_rows, self.col(number)]
        self.live.append(self.go(block, block, self.sibling, self.grp))

    def gather_second(self):
        for k in range(3):
            for copies in self.far:
                copies[k].wait_recv()
            self.share(lax.rem(self.mine0 + 3 - k, 4))

    def advance(self):
        levels = len(self.along_z)
        steps = [self.swap_start, self.swap_finish, self.scatter_second, self.z_start]
        for level in range(1, levels):
            steps.append(functools.partial(self.z_next, level))
        steps += [self.gather_start, self.gather_first, self.gather_second, self.land]
        steps[self.step]()
        self.step += 1

    def finish(self):
        for copy in self.started:
            copy.wait_send()


def halves(total):
    low = -(-total // (2 * 64)) * 64
    return [(0, low), (low, total - low)]


def kernel(
    block_owner,
    block_local,
    table_hbm,
    phases,
    head_ids,
    rel_ids,
    target_pos,
    losses_out,
    head_any,
    grads_any,
    c_acc,
    cs_stage,
    cs_recv,
    cands,
    g_acc,
    g_stage,
    grads,
    s_stage,
    s_recv,
    c_r0,
    c_r1,
    c_rz,
    g_r0,
    g_r1,
    g_rz2,
    g_rz4,
    table,
    loaded,
    padded,
    queries,
    head_out,
    local_sem,
    send,
    recv,
):
    ent = lax.axis_index("ent")
    grp = lax.axis_index("grp")
    core = lax.rem(ent, 2)
    sibling = ent + 1 - 2 * core
    zlo = lax.rem(ent // 2, 4)
    plane = ent - 2 * zlo
    half = phases.shape[1]
    rel_count = phases.shape[0]
    rel_half = padded.shape[0] // 2
    n_cand = c_acc.shape[0]
    blocks = n_cand // BLK
    q_dev = head_ids.shape[1]

    first = pltpu.make_async_copy(table_hbm, table, local_sem.at[5])
    first.start()
    load = pltpu.make_async_copy(phases, loaded, local_sem.at[0])
    load.start()
    barrier = pltpu.get_barrier_semaphore()
    partners = [(sibling, grp), (ent, 1 - grp)]
    for stride, size in (XDIM, YDIM, ZLO):
        mine = lax.rem(ent // stride, size)
        for s in range(1, size):
            partners.append((ent + (lax.rem(mine + s, size) - mine) * stride, grp))
    across = plane + 2 * lax.rem(zlo + 2, 4)
    partners.append((across, 1 - grp))
    for partner in partners:
        pl.semaphore_signal(barrier, inc=1, device_id=partner, device_id_type=MESH)

    first.wait()
    for b in range(blocks):
        for side, target in ((core, c_acc), (1 - core, cs_stage)):
            columns = pl.ds(pl.multiple_of(side * half, 128), half)
            total = jnp.zeros((BLK, half), BF16)
            for local in range(table.shape[0] // BLK):
                wanted = jnp.logical_and(block_owner[b] == ent, block_local[b] == local)
                total = jnp.where(wanted, table[pl.ds(local * BLK, BLK), columns], total)
            target[pl.ds(b * BLK, BLK), :] = total

    pl.semaphore_wait(barrier, len(partners))

    place = (ent, grp)
    sems = ((send, []), recv)
    near_z = [(plane + 2 * lax.rem(zlo + s, 4), grp) for s in range(1, 4)]
    refs = (c_acc, c_acc, cands, (cs_stage, cs_recv), c_r0, c_r1, (c_rz,))
    fetch = [
        Exchange(refs, low, n_cand // 2, i, sems, place, [(zlo, near_z)])
        for i, low in enumerate((0, n_cand // 2))
    ]

    def advance(group):
        for exchange in group:
            exchange.advance()

    advance(fetch)

    rows_t = lax.broadcasted_iota(jnp.int32, (table.shape[0], q_dev), 0)
    head_pick = (rows_t == head_ids[...]).astype(F32).T.astype(BF16)
    heads = jnp.dot(head_pick, table[...], preferred_element_type=F32)
    rel_rows = lax.broadcasted_iota(jnp.int32, (2 * rel_half, q_dev), 0)
    rel_pick = (rel_rows == rel_ids[...]).astype(F32).T.astype(BF16)

    advance(fetch)

    load.wait()
    padded[...] = jnp.zeros_like(padded)
    padded[pl.ds(0, rel_count), :] = loaded[...]

    advance(fetch)

    whole = padded[...]
    top_part = whole.astype(BF16)
    left = whole - top_part.astype(F32)
    mid_part = left.astype(BF16)
    low_part = (left - mid_part.astype(F32)).astype(BF16)
    angles = (
        jnp.dot(rel_pick, low_part, preferred_element_type=F32)
        + jnp.dot(rel_pick, mid_part, preferred_element_type=F32)
    ) + jnp.dot(rel_pick, top_part, preferred_element_type=F32)

    advance(fetch)

    cosine = jnp.cos(angles)
    sine = jnp.sin(angles)

    advance(fetch)

    real_head = heads[:, :half]
    imag_head = heads[:, half:]
    real_query = real_head * cosine - imag_head * sine
    imag_query = real_head * sine + imag_head * cosine
    queries[0] = real_query.astype(BF16)
    queries[1] = imag_query.astype(BF16)

    for _ in range(2):
        advance(fetch)

    contract_last = (((1,), (1,)), ((), ()))
    inner = lax.dot_general(
        cands[core], queries[core], contract_last, preferred_element_type=F32
    )

    advance(fetch)

    inner = inner + lax.dot_general(
        cands[1 - core], queries[1 - core], contract_last, preferred_element_type=F32
    )
    cand_real = cands[0]
    cand_imag = cands[1]
    norm = jnp.sum(jnp.square(cand_real.astype(F32)), axis=1, keepdims=True)
    norm = norm + jnp.sum(jnp.square(cand_imag.astype(F32)), axis=1, keepdims=True)
    scores = (2.0 * inner - norm) / SOFTMAX_TEMPER
    top = jnp.max(scores, axis=0, keepdims=True)
    log_total = top + jnp.log(jnp.sum(jnp.exp(scores - top), axis=0, keepdims=True))
    target = lax.broadcasted_iota(jnp.int32, (n_cand, q_dev), 0) == target_pos[...]
    losses_out[...] = log_total - jnp.sum(jnp.where(target, scores, 0.0), axis=0, keepdims=True)
    weights = jnp.exp(scores - log_total) - target.astype(F32)
    weights_low = weights.astype(BF16)
    weight_sums = jnp.sum(weights, axis=1, keepdims=True)
    weights_by_query = weights.T.astype(BF16)
    scale = 2.0 / SOFTMAX_TEMPER

    def cand_part(side):
        return scale * (
            jnp.dot(weights_low, queries[side], preferred_element_type=F32)
            - weight_sums * cands[side].astype(F32)
        )

    refs = (g_acc, g_stage, grads, (s_stage, s_recv), g_r0, g_r1, (g_rz2, g_rz4))
    parity = lax.rem(zlo, 2)
    pair = (plane + 2 * (zlo + 1 - 2 * parity), grp)
    far_z = [(across, grp), (ent, 1 - grp), (across, 1 - grp)]
    along_z = [(parity, [pair]), (2 * grp + zlo // 2, far_z)]
    cand_reduce = [
        Exchange(refs, low, n_cand // 2, i, sems, place, along_z)
        for i, low in enumerate((0, n_cand // 2))
    ]
    rel_reduce = [
        Exchange(refs, n_cand + low, length, i, sems, place, along_z)
        for i, (low, length) in enumerate(halves(rel_half))
    ]

    s_stage[pl.ds(0, n_cand), :] = cand_part(1 - core).astype(BF16)
    advance(cand_reduce)
    g_acc[pl.ds(0, n_cand), :] = cand_part(core)
    advance(cand_reduce)

    real_grad = scale * jnp.dot(weights_by_query, cand_real, preferred_element_type=F32)
    imag_grad = scale * jnp.dot(weights_by_query, cand_imag, preferred_element_type=F32)
    angle_grad = imag_grad * real_query - real_grad * imag_query
    angle_high = angle_grad.astype(BF16)
    angle_low = (angle_grad - angle_high.astype(F32)).astype(BF16)

    def rel_part(side):
        rows = lax.broadcasted_iota(jnp.int32, (rel_half, q_dev), 0) + side * rel_half
        pick = (rows == rel_ids[...]).astype(F32).astype(BF16)
        return jnp.dot(pick, angle_high, preferred_element_type=F32) + jnp.dot(
            pick, angle_low, preferred_element_type=F32
        )

    s_stage[pl.ds(n_cand, rel_half), :] = rel_part(1 - core).astype(BF16)
    advance(rel_reduce)
    g_acc[pl.ds(n_cand, rel_half), :] = rel_part(core)
    advance(cand_reduce)
    advance(rel_reduce)

    head_out[:, pl.ds(0, half)] = (real_grad * cosine + imag_grad * sine).astype(BF16)
    head_out[:, pl.ds(half, half)] = (imag_grad * cosine - real_grad * sine).astype(BF16)
    stores = []

    def store(src, dst):
        copy = pltpu.make_async_copy(src, dst, local_sem.at[1 + len(stores)])
        copy.start()
        stores.append(copy)

    store(head_out, head_any)
    while cand_reduce[0].step < 9:
        advance(cand_reduce)
        advance(rel_reduce)
    block = pl.ds(0, n_cand)
    store(grads.at[:, block, :], grads_any.at[:, block, :])
    while rel_reduce[0].step < 9:
        advance(rel_reduce)
    block = pl.ds(n_cand, rel_half)
    store(grads.at[:, block, :], grads_any.at[:, block, :])
    for exchange in fetch + cand_reduce + rel_reduce:
        exchange.finish()
    for copy in stores:
        copy.wait()


def finish(
    block_owner,
    block_local,
    losses_in,
    head_in,
    grads_in,
    losses_out,
    head_out,
    table_out,
    rel_out,
    losses,
    head,
    grads,
    table,
    rel,
    sem,
):
    ent = lax.axis_index("ent")
    blocks = block_owner.shape[0]
    n_cand = blocks * BLK
    rel_half = grads.shape[1] - n_cand
    half = grads.shape[2]
    begun = []

    def copy(src, dst):
        begun.append(pltpu.make_async_copy(src, dst, sem.at[len(begun)]))
        begun[-1].start()
        return begun[-1]

    cand_rows, rel_rows = pl.ds(0, n_cand), pl.ds(n_cand, rel_half)
    cand_load = copy(grads_in.at[:, cand_rows, :], grads.at[:, cand_rows, :])
    rel_load = copy(grads_in.at[:, rel_rows, :], grads.at[:, rel_rows, :])
    head_load = copy(head_in, head)
    losses_load = copy(losses_in, losses)
    stores = []
    cand_load.wait()
    for local in range(table.shape[0] // BLK):
        rows = pl.ds(local * BLK, BLK)
        for side in range(2):
            total = jnp.zeros((BLK, half), F32)
            for b in range(blocks):
                mine = jnp.logical_and(block_owner[b] == ent, block_local[b] == local)
                value = grads[side, pl.ds(b * BLK, BLK), :].astype(F32)
                total = total + jnp.where(mine, value, 0.0)
            table[rows, pl.ds(side * half, half)] = total.astype(BF16)
        stores.append(copy(table.at[rows, :], table_out.at[rows, :]))
    rel_load.wait()
    tail = rel.shape[0] - rel_half
    rel[pl.ds(0, rel_half), :] = grads[0, rel_rows, :].astype(F32)
    rel[pl.ds(rel_half, tail), :] = grads[1, rel_rows, :].astype(F32)[:tail]
    stores.append(copy(rel, rel_out))
    head_load.wait()
    stores.append(copy(head, head_out))
    losses_load.wait()
    stores.append(copy(losses, losses_out))
    for one in stores:
        one.wait()


def body(entity_table, rel_phases, head_ids, rel_ids, target_pos, block_owner, block_local):
    rel_count, half = rel_phases.shape
    shard_rows = entity_table.shape[0]
    q_dev = head_ids.shape[0]
    n_cand = block_owner.shape[0] * BLK
    rel_half = -(-rel_count // (2 * 64)) * 64
    g_rows = n_cand + rel_half
    copies = 2 * 29 + 4 * 30

    def slots(count, rows):
        return pltpu.VMEM((count, rows, TILE), BF16)

    vmem = pl.BlockSpec(memory_space=pltpu.VMEM)
    smem = pl.BlockSpec(memory_space=pltpu.SMEM)
    anywhere = pl.BlockSpec(memory_space=pl.ANY)
    hbm = pl.BlockSpec(memory_space=pltpu.HBM)
    losses_type = jax.ShapeDtypeStruct((1, q_dev), F32)
    head_type = jax.ShapeDtypeStruct((q_dev, 2 * half), BF16)
    raw = pl.pallas_call(
        kernel,
        out_shape=(losses_type, head_type, jax.ShapeDtypeStruct((2, g_rows, half), BF16)),
        in_specs=[smem, smem, hbm, hbm] + [vmem] * 3,
        out_specs=(vmem, anywhere, anywhere),
        scratch_shapes=[
            pltpu.VMEM((n_cand, half), BF16),
            pltpu.VMEM((n_cand, half), BF16),
            pltpu.VMEM((n_cand, half), BF16),
            pltpu.VMEM((2, n_cand, half), BF16),
            pltpu.VMEM((g_rows, half), F32),
            pltpu.VMEM((g_rows, half), BF16),
            pltpu.VMEM((2, g_rows, half), BF16),
            pltpu.VMEM((g_rows, half), BF16),
            pltpu.VMEM((g_rows, half), BF16),
            slots(3, n_cand),
            slots(3, n_cand // 4),
            slots(4, n_cand // 4),
            slots(3, g_rows),
            slots(3, g_rows // 4),
            slots(2, g_rows // 4),
            slots(4, g_rows // 4),
            pltpu.VMEM((shard_rows, 2 * half), BF16),
            pltpu.VMEM((rel_count, half), F32),
            pltpu.VMEM((2 * rel_half, half), F32),
            pltpu.VMEM((2, q_dev, half), BF16),
            pltpu.VMEM((q_dev, 2 * half), BF16),
            pltpu.SemaphoreType.DMA((6,)),
            pltpu.SemaphoreType.DMA((copies,)),
            pltpu.SemaphoreType.DMA((copies,)),
        ],
        compiler_params=pltpu.CompilerParams(collective_id=0, has_side_effects=True),
    )(
        block_owner,
        block_local,
        entity_table,
        rel_phases,
        head_ids.reshape(1, q_dev),
        rel_ids.reshape(1, q_dev),
        target_pos.reshape(1, q_dev),
    )
    table_type = jax.ShapeDtypeStruct((shard_rows, 2 * half), BF16)
    rel_type = jax.ShapeDtypeStruct((rel_count, half), F32)
    losses, head_grad, table_grad, rel_grad = pl.pallas_call(
        finish,
        out_shape=(losses_type, head_type, table_type, rel_type),
        in_specs=[smem, smem] + [anywhere] * 3,
        out_specs=(anywhere,) * 4,
        scratch_shapes=[
            pltpu.VMEM((1, q_dev), F32),
            pltpu.VMEM((q_dev, 2 * half), BF16),
            pltpu.VMEM((2, g_rows, half), BF16),
            pltpu.VMEM((shard_rows, 2 * half), BF16),
            pltpu.VMEM((rel_count, half), F32),
            pltpu.SemaphoreType.DMA((7 + shard_rows // BLK,)),
        ],
    )(block_owner, block_local, *raw)
    return losses.reshape(q_dev), head_grad, table_grad, rel_grad


def solution(mesh):
    return jax.shard_map(
        body,
        mesh=mesh,
        in_specs=(
            P("ent", None),
            P(),
            P(("ent", "grp")),
            P(("ent", "grp")),
            P(("ent", "grp")),
            P(),
            P(),
        ),
        out_specs=(P(("ent", "grp")), P(("ent", "grp"), None), P("ent", None), P()),
        check_vma=False,
    )
```
